32 devices in a mesh: fsdp: 8 (over z, x), tp: 4 (over y, core).
Axes of the slice: x: 2, y: 2, z: 4, core: 2. Of those that a mesh axis runs over, the one named last changes fastest.
Arguments:
- master: float32 [256, 8192], P('fsdp', 'tp'), may hold values from -0.0625 to 0.0625
- first_moment: float32 [256, 8192], P('fsdp', 'tp'), may hold values from -0.008286407 to 0.008286407
- second_moment: float32 [256, 8192], P('fsdp', 'tp'), may hold values from 2.3841858e-07 to 9.536743e-06
- gradients: float32 [256, 8192], P('fsdp', 'tp'), as said below
- step_count: int32 [1], replicated, may hold values from 1 to 8
- tile_round: int32 [32], replicated, may hold values from 0 to 3, as said below
Outputs:
- new_master: float32 [256, 8192], P('fsdp', 'tp')
- new_first: float32 [256, 8192], P('fsdp', 'tp')
- new_second: float32 [256, 8192], P('fsdp', 'tp')
- weights: bfloat16 [256, 8192], P(None, 'tp')
The draws below stay inside these ranges and needn't reach their ends.
Inputs may be any that keep to these rules, and one draw needn't show every extreme that they name: `tile_round`: each aligned block of 4 entries (the tiles of one index of fsdp) holds every round number 0 to 3 exactly once. `gradients`: exactly one entry has magnitude 1000 or more; every other entry has magnitude under 100, and in every round without that entry the sum of squares is under 1e5.
All inputs are finite; a program needn't handle non-finite values.
Results may differ from the reference program's by a relative error of at most 0.001.
Values may be sent and summed in bfloat16 or wider, within the bound.
A program may use at most 64 MiB of HBM per device.

```python
import math
import jax
import jax.numpy as jnp

COLS = 8192
TILE_ROWS = 8
ROUNDS = 4
ROWS_DEV = 32
ROWS = 256
TILES = 32


def round_labels(key):
    blocks = ROWS // ROWS_DEV
    scores = jax.random.randint(jax.random.fold_in(key, 7), (blocks, ROUNDS), 0, 2 ** 30)
    order = jnp.argsort(scores, axis=1, stable=True).astype(jnp.int32)
    return order.reshape(TILES)


def draw_gradients(key, part):
    labels = round_labels(key)
    keys = jax.random.split(jax.random.fold_in(key, 29), 7)
    base = jax.random.normal(keys[0], (ROWS, COLS), jnp.float32)
    row_scale = jnp.exp(jax.random.uniform(keys[1], (ROWS, 1), jnp.float32, 0.0, math.log(10.0)))
    low_lo, low_hi, high_lo, high_hi = (0.05, 0.5, 2.0, 40.0)
    row_ids = jnp.arange(ROWS, dtype=jnp.int32).reshape(ROWS, 1)
    col_ids = jnp.arange(COLS, dtype=jnp.int32).reshape(1, COLS)
    blocks = ROWS // ROWS_DEV
    row_rise = 1.0 + 2.0 * (row_ids // ROWS_DEV).astype(jnp.float32) / max(blocks - 1, 1)
    col_rise = 1.0 + 2.0 * col_ids.astype(jnp.float32) / max(COLS - 1, 1)
    values = base * row_scale * row_rise * col_rise
    row_round = jnp.repeat(labels, TILE_ROWS).reshape(ROWS, 1)
    onehot = (row_round == jnp.arange(ROUNDS, dtype=jnp.int32).reshape(1, ROUNDS)).astype(jnp.float32)
    row_squares = jnp.sum(values * values, axis=1)
    round_squares = jnp.sum(onehot * row_squares.reshape(ROWS, 1), axis=0)
    shuffled = jax.random.permutation(keys[5], ROUNDS)
    is_low = shuffled < ROUNDS // 2
    fraction = jax.random.uniform(keys[6], (ROUNDS,), jnp.float32, 0.0, 1.0)
    low_target = jnp.exp(math.log(low_lo) + fraction * (math.log(low_hi) - math.log(low_lo)))
    high_target = jnp.exp(math.log(high_lo) + fraction * (math.log(high_hi) - math.log(high_lo)))
    target = jnp.where(is_low, low_target, high_target)
    factor = jnp.sqrt(target / round_squares)
    row_factor = jnp.sum(onehot * factor.reshape(1, ROUNDS), axis=1)
    values = values * row_factor.reshape(ROWS, 1)
    pick_row = jax.random.randint(keys[2], (), 0, ROWS)
    pick_col = jax.random.randint(keys[3], (), 0, COLS)
    spot = jnp.logical_and(row_ids == pick_row, col_ids == pick_col)
    return jnp.where(spot, jnp.float32(5000.0), values).astype(jnp.float32)


def draw_tile_round(key, part):
    return round_labels(key)


def steps_of(rng, extent, cuts, smallest, high):
    loudness, own = 1.0, jax.random.fold_in(rng, 6)
    for position, shards_of in cuts:
        draws = jnp.exp(jax.random.uniform(jax.random.fold_in(own, position), (shards_of,), jnp.float32, smallest / len(cuts), high / len(cuts)))
        loudness = loudness * jnp.repeat(draws, extent[position] // shards_of).reshape([-1 if axis == position else 1 for axis in range(len(extent))])
    return loudness


def normal_values(own_key, shape, deviation, limit, shards=(), kind=jnp.bfloat16):
    gain = steps_of(own_key, shape, shards, -0.22, 0.18) if shards else 1.0
    array = jax.random.normal(own_key, shape, jnp.float32) * deviation * gain
    return jnp.minimum(jnp.maximum(array, -limit), limit).astype(kind)


def setup_inputs(seed: int = 0) -> dict:
    key_list = jax.random.split(jax.random.key(seed), 7)
    return {
        "master": normal_values(key_list[0], (ROWS, COLS), COLS ** -0.5, 0.0625, ((0, 8), (1, 4)), jnp.float32),
        "first_moment": normal_values(key_list[1], (ROWS, COLS), (2.0 * (ROWS * COLS) ** (-0.5)), 0.008286407, ((0, 8), (1, 4)), jnp.float32),
        "second_moment": jnp.clip(jnp.exp(math.log(9.5367431640625e-06) - 3.6888795 * jax.random.uniform(key_list[2], (ROWS, COLS), jnp.float32) ** steps_of(key_list[2], (ROWS, COLS), ((0, 8), (1, 4)), -0.2, 0.2)), 2.384185791015625e-07, 9.5367431640625e-06),
        "gradients": draw_gradients(jax.random.fold_in(key_list[6], 71), 0),
        "step_count": jax.random.randint(key_list[4], (1,), 1, 9).astype(jnp.int32),
        "tile_round": draw_tile_round(jax.random.fold_in(key_list[6], 71), 0),
    }


beta_one = 0.9
beta_two = 0.95
adam_epsilon = 1e-08
learning_rate = 0.01
weight_decay = 0.1
clip_norm = 1.0
overflow_limit = 1000.0

def reference(master, first_moment, second_moment, gradients, step_count, tile_round):
    row_count, columns = master.shape
    tile_count = tile_round.shape[0]
    shaped = (tile_count, row_count // tile_count, columns)
    params = master.reshape(shaped)
    moment_one = first_moment.reshape(shaped)
    moment_two = second_moment.reshape(shaped)
    grads = gradients.reshape(shaped)
    labels = tile_round.reshape(tile_count, 1, 1)
    steps = step_count[0].astype(jnp.float32)
    correct_one = 1.0 - jnp.power(jnp.float32(beta_one), steps)
    correct_two = 1.0 - jnp.power(jnp.float32(beta_two), steps)
    out_p, out_m, out_v = (params, moment_one, moment_two)
    for round_index in range(ROUNDS):
        inside = labels == round_index
        total = jnp.sum(jnp.where(inside, grads * grads, jnp.float32(0.0)))
        overflow = jnp.logical_and(inside, jnp.abs(grads) >= overflow_limit)
        broken = jnp.max(jnp.where(overflow, jnp.int32(1), jnp.int32(0)))
        scale = jnp.minimum(jnp.float32(1.0), clip_norm / (jnp.sqrt(total) + 1e-06))
        clipped = grads * scale
        moment_new = beta_one * moment_one + (1.0 - beta_one) * clipped
        second_new = beta_two * moment_two + (1.0 - beta_two) * clipped * clipped
        ratio = moment_new / correct_one / (jnp.sqrt(second_new / correct_two) + adam_epsilon)
        param_new = params - learning_rate * (ratio + weight_decay * params)
        apply = jnp.logical_and(inside, broken == 0)
        out_p = jnp.where(apply, param_new, out_p)
        out_m = jnp.where(apply, moment_new, out_m)
        out_v = jnp.where(apply, second_new, out_v)
    new_master = out_p.reshape(row_count, columns)
    return (new_master, out_m.reshape(row_count, columns), out_v.reshape(row_count, columns), new_master.astype(jnp.bfloat16))
```

```python
import functools

import jax
import jax.numpy as jnp
from jax import lax
from jax.experimental import pallas as pl
from jax.experimental.pallas import tpu as pltpu
from jax.sharding import PartitionSpec as P

ROUNDS = 4
LANES = 128
MESH = pl.DeviceIdType.MESH

beta_one = 0.9
beta_two = 0.95
adam_epsilon = 1e-08
learning_rate = 0.01
weight_decay = 0.1
clip_norm = 1.0
square_limit = 1000000.0


def plan(fsdp, columns):
    if fsdp > 16 or columns % (16 * LANES):
        return [(0, columns, False)]
    unit = columns // 16
    chunks, start = [], 0
    for index, units in enumerate((3, 3, 3, 3, 4)):
        chunks.append((start, units * unit, index == 0))
        start += units * unit
    return chunks


def kernel(fsdp, tp, chunks, g_hbm, p_hbm, m_hbm, v_hbm, step_ref, round_ref,
           p_out, m_out, v_out, w_out,
           g_ref, p_ref, m_ref, v_ref, own_a, slots_a, own_b, slots_b,
           load_sem, sa_sem, ra_sem, sb_sem, rb_sem, up_sem, down_sem, side_sem, recv_sem):
    line = fsdp // 2
    f = lax.axis_index("fsdp")
    t = lax.axis_index("tp")
    a = f // 2
    b = f % 2
    rows, columns = g_ref.shape
    tile = rows // ROUNDS

    group = [(db, dt) for db in range(2) for dt in range(tp) if (db, dt) != (0, 0)]

    def peer_a(db, dt):
        return (a * 2 + (b + db) % 2, (t + dt) % tp)

    def peer_b(d):
        return (((a + d) % line) * 2 + b, t)

    loads = [pltpu.make_async_copy(src, dst, load_sem.at[i]) for i, (src, dst) in enumerate(
        ((g_hbm, g_ref), (p_hbm, p_ref), (m_hbm, m_ref), (v_hbm, v_ref)))]
    loads[0].start()
    barrier = pltpu.get_barrier_semaphore()
    for d in range(1, line):
        pl.semaphore_signal(barrier, inc=1, device_id=peer_b(d), device_id_type=MESH)
    for db, dt in group:
        pl.semaphore_signal(barrier, inc=1, device_id=peer_a(db, dt), device_id_type=MESH)
    for load in loads[1:]:
        load.start()

    row_ids = lax.broadcasted_iota(jnp.int32, (8, LANES), 0)
    mine = [round_ref[f * ROUNDS + k] for k in range(ROUNDS)]
    loads[0].wait()
    payload = jnp.zeros((8, LANES), jnp.float32)
    for k in range(ROUNDS):
        part = jnp.zeros((tile, LANES), jnp.float32)
        for c in range(columns // LANES):
            piece = g_ref[k * tile:(k + 1) * tile, c * LANES:(c + 1) * LANES]
            part = part + piece * piece
        part = jnp.sum(part, axis=0, keepdims=True)
        payload = payload + jnp.where(row_ids == mine[k], part, 0.0)
    own_a[...] = payload
    pl.semaphore_wait(barrier, len(group) + line - 1)

    sends_a = []
    for i, (db, dt) in enumerate(group):
        sends_a.append(pltpu.make_async_remote_copy(
            src_ref=own_a, dst_ref=slots_a.at[i], send_sem=sa_sem.at[i], recv_sem=ra_sem.at[i],
            device_id=peer_a(db, dt), device_id_type=MESH))
        sends_a[-1].start()
    for load in loads[1:]:
        load.wait()
    steps = jnp.full((1, LANES), step_ref[0].astype(jnp.float32), jnp.float32)
    inverse_one = 1.0 / (1.0 - jnp.exp(steps * jnp.log(jnp.float32(beta_one))))
    inverse_two = 1.0 / (1.0 - jnp.exp(steps * jnp.log(jnp.float32(beta_two))))
    inverse_one = inverse_one[:, :1]
    inverse_two = inverse_two[:, :1]
    total = payload
    for i, copy in enumerate(sends_a):
        copy.wait_recv()
        total = total + slots_a[i]
    own_b[...] = total
    sends_b = []
    for d in range(1, line):
        sends_b.append(pltpu.make_async_remote_copy(
            src_ref=own_b, dst_ref=slots_b.at[d - 1], send_sem=sb_sem.at[d - 1], recv_sem=rb_sem.at[d - 1],
            device_id=peer_b(d), device_id_type=MESH))
        sends_b[-1].start()
    for d, copy in enumerate(sends_b):
        copy.wait_recv()
        total = total + slots_b[d]

    scales, keeps = [], []
    for k in range(ROUNDS):
        picked = jnp.sum(jnp.where(row_ids == mine[k], total, 0.0), axis=0, keepdims=True)
        picked = jnp.sum(picked, axis=1, keepdims=True)
        keeps.append(picked >= square_limit)
        scales.append(jnp.minimum(1.0, clip_norm / (jnp.sqrt(picked) + 1e-06)))

    def block_of(row, c):
        start, width, _ = chunks[c]
        return w_out.at[pl.ds(pl.multiple_of(row * rows, rows), rows), pl.ds(start, width)]

    def send(row, c, sems, target):
        return pltpu.make_async_remote_copy(
            src_ref=block_of(row, c), dst_ref=block_of(row, c), send_sem=sems.at[row, c],
            recv_sem=recv_sem.at[row, c], device_id=(target, t), device_id_type=MESH)

    side = a * 2 + (1 - b)
    above, below = a < line - 1, a > 0

    def up(row, c):
        return send(row, c, up_sem, f + 2)

    def down(row, c):
        return send(row, c, down_sem, f - 2)

    def across(row, c):
        return send(row, c, side_sem, side)

    def when_do(condition, make, method):
        @pl.when(condition)
        def _():
            getattr(make(), method)()

    sent = []

    def go(condition, make):
        when_do(condition, make, "start")
        sent.append((condition, make))

    always = a >= 0
    for c, (start, width, first) in enumerate(chunks):
        for k in range(ROUNDS):
            at = (slice(k * tile, (k + 1) * tile), slice(start, start + width))
            old_p, old_m, old_v = p_ref[at], m_ref[at], v_ref[at]
            clipped = g_ref[at] * scales[k]
            moment = beta_one * old_m + (1.0 - beta_one) * clipped
            second = beta_two * old_v + (1.0 - beta_two) * clipped * clipped
            ratio = moment * inverse_one / (jnp.sqrt(second * inverse_two) + adam_epsilon)
            param = old_p - learning_rate * (ratio + weight_decay * old_p)
            param = jnp.where(keeps[k], old_p, param)
            p_out[at] = param
            m_out[at] = jnp.where(keeps[k], old_m, moment)
            v_out[at] = jnp.where(keeps[k], old_v, second)
        own_rows = pl.ds(pl.multiple_of(f * rows, rows), rows)
        w_out[own_rows, start:start + width] = p_out[:, start:start + width].astype(jnp.bfloat16)
        go(always, functools.partial(across, f, c))
        go(above, functools.partial(up, f, c))
        go(below, functools.partial(down, f, c))

    for c, (_, _, first) in enumerate(chunks):
        if first:
            across(side, c).wait_recv()
            go(above, functools.partial(up, side, c))
            go(below, functools.partial(down, side, c))

    for d in range(1, line):
        for c, (_, _, first) in enumerate(chunks):
            for from_below in (True, False):
                inside = (a >= d) if from_below else (a + d <= line - 1)
                onward = above if from_below else below
                shift = -2 * d if from_below else 2 * d
                for adopted in ((False, True) if first else (False,)):
                    row = (side if adopted else f) + shift
                    make = functools.partial(up if from_below else down, row, c)
                    when_do(inside, make, "wait_recv")
                    go(jnp.logical_and(inside, onward), make)
                    if not first:
                        go(inside, functools.partial(across, row, c))

    for c, (_, _, first) in enumerate(chunks):
        if not first:
            across(side, c).wait_recv()
    for d in range(1, line):
        for c, (_, _, first) in enumerate(chunks):
            if not first:
                when_do(a >= d, functools.partial(across, side - 2 * d, c), "wait_recv")
                when_do(a + d <= line - 1, functools.partial(across, side + 2 * d, c), "wait_recv")

    for copy in sends_a + sends_b:
        copy.wait_send()
    for condition, make in sent:
        when_do(condition, make, "wait_send")


def solution(mesh):
    fsdp, tp = mesh.shape["fsdp"], mesh.shape["tp"]

    def local(master, first_moment, second_moment, gradients, step_count, tile_round):
        rows, columns = master.shape
        chunks = plan(fsdp, columns)
        count = len(chunks)
        line = fsdp // 2
        shape = jax.ShapeDtypeStruct((rows, columns), jnp.float32)
        sems = pltpu.SemaphoreType.DMA
        block = pltpu.VMEM((rows, columns), jnp.float32)
        p, m, v, w = pl.pallas_call(
            functools.partial(kernel, fsdp, tp, chunks),
            out_shape=(shape, shape, shape, jax.ShapeDtypeStruct((fsdp * rows, columns), jnp.bfloat16)),
            in_specs=[pl.BlockSpec(memory_space=pltpu.HBM)] * 4 + [pl.BlockSpec(memory_space=pltpu.SMEM)] * 2,
            out_specs=[pl.BlockSpec(memory_space=pltpu.VMEM)] * 4,
            scratch_shapes=[
                block, block, block, block,
                pltpu.VMEM((8, LANES), jnp.float32),
                pltpu.VMEM((2 * tp - 1, 8, LANES), jnp.float32),
                pltpu.VMEM((8, LANES), jnp.float32),
                pltpu.VMEM((line - 1, 8, LANES), jnp.float32),
                sems((4,)), sems((2 * tp - 1,)), sems((2 * tp - 1,)), sems((line - 1,)), sems((line - 1,)),
                sems((fsdp, count)), sems((fsdp, count)), sems((fsdp, count)), sems((fsdp, count)),
            ],
            compiler_params=pltpu.CompilerParams(
                collective_id=0, has_side_effects=True, vmem_limit_bytes=40 * 1024 * 1024),
        )(gradients, master, first_moment, second_moment, step_count, tile_round)
        return p, m, v, w

    return jax.shard_map(
        local,
        mesh=mesh,
        in_specs=(P("fsdp", "tp"), P("fsdp", "tp"), P("fsdp", "tp"), P("fsdp", "tp"), P(), P()),
        out_specs=(P("fsdp", "tp"), P("fsdp", "tp"), P("fsdp", "tp"), P(None, "tp")),
        check_vma=False,
    )
```

```python
import functools

import jax
import jax.numpy as jnp
from jax import lax
from jax.experimental import pallas as pl
from jax.experimental.pallas import tpu as pltpu
from jax.sharding import PartitionSpec as P

ROUNDS = 4
LANES = 128
MESH = pl.DeviceIdType.MESH

beta_one = 0.9
beta_two = 0.95
adam_epsilon = 1e-08
learning_rate = 0.01
weight_decay = 0.1
clip_norm = 1.0
square_limit = 1000000.0


def plan(fsdp, columns):
    if fsdp > 16 or columns % (16 * LANES):
        return [(0, columns, False)]
    unit = columns // 16
    chunks, start = [], 0
    for index, units in enumerate((4, 4, 4, 4)):
        chunks.append((start, units * unit, False))
        start += units * unit
    return chunks


def kernel(fsdp, tp, chunks, g_hbm, p_hbm, m_hbm, v_hbm, step_hbm, round_hbm,
           p_out, m_out, v_out, w_out,
           g_ref, p_ref, m_ref, v_ref, own_a, slots_a, own_b, slots_b,
           step_ref, round_ref, load_sem, sa_sem, ra_sem, sb_sem, rb_sem, up_sem, down_sem, side_sem, recv_sem):
    line = fsdp // 2
    f = lax.axis_index("fsdp")
    t = lax.axis_index("tp")
    a = f // 2
    b = f % 2
    rows, columns = g_ref.shape
    tile = rows // ROUNDS

    group = [(db, dt) for db in range(2) for dt in range(tp) if (db, dt) != (0, 0)]

    def peer_a(db, dt):
        return (a * 2 + (b + db) % 2, (t + dt) % tp)

    def peer_b(d):
        return (((a + d) % line) * 2 + b, t)

    loads = [pltpu.make_async_copy(src, dst, load_sem.at[i]) for i, (src, dst) in enumerate(
        ((g_hbm, g_ref), (round_hbm, round_ref), (step_hbm, step_ref),
         (p_hbm, p_ref), (m_hbm, m_ref), (v_hbm, v_ref)))]
    loads[0].start()
    barrier = pltpu.get_barrier_semaphore()
    for d in range(1, line):
        pl.semaphore_signal(barrier, inc=1, device_id=peer_b(d), device_id_type=MESH)
    for db, dt in group:
        pl.semaphore_signal(barrier, inc=1, device_id=peer_a(db, dt), device_id_type=MESH)
    for load in loads[1:]:
        load.start()

    row_ids = lax.broadcasted_iota(jnp.int32, (8, LANES), 0)
    loads[1].wait()
    mine = [round_ref[f * ROUNDS + k] for k in range(ROUNDS)]
    loads[0].wait()
    payload = jnp.zeros((8, LANES), jnp.float32)
    for k in range(ROUNDS):
        part = jnp.zeros((tile, LANES), jnp.float32)
        for c in range(columns // LANES):
            piece = g_ref[k * tile:(k + 1) * tile, c * LANES:(c + 1) * LANES]
            part = part + piece * piece
        part = jnp.sum(part, axis=0, keepdims=True)
        payload = payload + jnp.where(row_ids == mine[k], part, 0.0)
    own_a[...] = payload
    pl.semaphore_wait(barrier, len(group) + line - 1)

    sends_a = []
    for i, (db, dt) in enumerate(group):
        sends_a.append(pltpu.make_async_remote_copy(
            src_ref=own_a, dst_ref=slots_a.at[i], send_sem=sa_sem.at[i], recv_sem=ra_sem.at[i],
            device_id=peer_a(db, dt), device_id_type=MESH))
        sends_a[-1].start()
    for load in loads[2:]:
        load.wait()
    steps = jnp.full((1, LANES), step_ref[0].astype(jnp.float32), jnp.float32)
    inverse_one = 1.0 / (1.0 - jnp.exp(steps * jnp.log(jnp.float32(beta_one))))
    inverse_two = 1.0 / (1.0 - jnp.exp(steps * jnp.log(jnp.float32(beta_two))))
    inverse_one = inverse_one[:, :1]
    inverse_two = inverse_two[:, :1]
    total = payload
    for i, copy in enumerate(sends_a):
        copy.wait_recv()
        total = total + slots_a[i]
    own_b[...] = total
    sends_b = []
    for d in range(1, line):
        sends_b.append(pltpu.make_async_remote_copy(
            src_ref=own_b, dst_ref=slots_b.at[d - 1], send_sem=sb_sem.at[d - 1], recv_sem=rb_sem.at[d - 1],
            device_id=peer_b(d), device_id_type=MESH))
        sends_b[-1].start()
    for d, copy in enumerate(sends_b):
        copy.wait_recv()
        total = total + slots_b[d]

    scales, keeps = [], []
    for k in range(ROUNDS):
        picked = jnp.sum(jnp.where(row_ids == mine[k], total, 0.0), axis=0, keepdims=True)
        picked = jnp.sum(picked, axis=1, keepdims=True)
        keeps.append(picked >= square_limit)
        scales.append(jnp.minimum(1.0, clip_norm / (jnp.sqrt(picked) + 1e-06)))

    def block_of(row, c):
        start, width, _ = chunks[c]
        return w_out.at[pl.ds(pl.multiple_of(row * rows, rows), rows), pl.ds(start, width)]

    def send(row, c, sems, target):
        return pltpu.make_async_remote_copy(
            src_ref=block_of(row, c), dst_ref=block_of(row, c), send_sem=sems.at[row, c],
            recv_sem=recv_sem.at[row, c], device_id=(target, t), device_id_type=MESH)

    side = a * 2 + (1 - b)
    above, below = a < line - 1, a > 0

    def up(row, c):
        return send(row, c, up_sem, f + 2)

    def down(row, c):
        return send(row, c, down_sem, f - 2)

    def across(row, c):
        return send(row, c, side_sem, side)

    def when_do(condition, make, method):
        @pl.when(condition)
        def _():
            getattr(make(), method)()

    sent = []

    def go(condition, make):
        when_do(condition, make, "start")
        sent.append((condition, make))

    always = a >= 0
    for c, (start, width, first) in enumerate(chunks):
        for k in range(ROUNDS):
            at = (slice(k * tile, (k + 1) * tile), slice(start, start + width))
            old_p, old_m, old_v = p_ref[at], m_ref[at], v_ref[at]
            clipped = g_ref[at] * scales[k]
            moment = beta_one * old_m + (1.0 - beta_one) * clipped
            second = beta_two * old_v + (1.0 - beta_two) * clipped * clipped
            ratio = moment * inverse_one / (jnp.sqrt(second * inverse_two) + adam_epsilon)
            param = old_p - learning_rate * (ratio + weight_decay * old_p)
            param = jnp.where(keeps[k], old_p, param)
            p_out[at] = param
            m_out[at] = jnp.where(keeps[k], old_m, moment)
            v_out[at] = jnp.where(keeps[k], old_v, second)
        own_rows = pl.ds(pl.multiple_of(f * rows, rows), rows)
        w_out[own_rows, start:start + width] = p_out[:, start:start + width].astype(jnp.bfloat16)
        go(always, functools.partial(across, f, c))
        go(above, functools.partial(up, f, c))
        go(below, functools.partial(down, f, c))

    for c, (_, _, first) in enumerate(chunks):
        if first:
            across(side, c).wait_recv()
            go(above, functools.partial(up, side, c))
            go(below, functools.partial(down, side, c))

    for d in range(1, line):
        passing = [(False, c) for c in range(len(chunks))]
        passing += [(True, c) for c, (_, _, first) in enumerate(chunks) if first]
        for adopted, c in passing:
            for from_below in (True, False):
                inside = (a >= d) if from_below else (a + d <= line - 1)
                onward = above if from_below else below
                row = (side if adopted else f) + (-2 * d if from_below else 2 * d)
                make = functools.partial(up if from_below else down, row, c)
                when_do(inside, make, "wait_recv")
                go(jnp.logical_and(inside, onward), make)
                if not (adopted or chunks[c][2]):
                    go(inside, functools.partial(across, row, c))

    for c, (_, _, first) in enumerate(chunks):
        if not first:
            across(side, c).wait_recv()
    for d in range(1, line):
        for c, (_, _, first) in enumerate(chunks):
            if not first:
                when_do(a >= d, functools.partial(across, side - 2 * d, c), "wait_recv")
                when_do(a + d <= line - 1, functools.partial(across, side + 2 * d, c), "wait_recv")

    for copy in sends_a + sends_b:
        copy.wait_send()
    for condition, make in sent:
        when_do(condition, make, "wait_send")


def put_out(*refs):
    sources, targets, sem = refs[:4], refs[4:8], refs[8]
    copies = [pltpu.make_async_copy(src, dst, sem.at[i]) for i, (src, dst) in enumerate(zip(sources, targets))]
    for copy in reversed(copies):
        copy.start()
    for copy in copies:
        copy.wait()


def solution(mesh):
    fsdp, tp = mesh.shape["fsdp"], mesh.shape["tp"]

    def local(master, first_moment, second_moment, gradients, step_count, tile_round):
        rows, columns = master.shape
        chunks = plan(fsdp, columns)
        count = len(chunks)
        line = fsdp // 2
        shape = jax.ShapeDtypeStruct((rows, columns), jnp.float32)
        sems = pltpu.SemaphoreType.DMA
        block = pltpu.VMEM((rows, columns), jnp.float32)
        p, m, v, w = pl.pallas_call(
            functools.partial(kernel, fsdp, tp, chunks),
            out_shape=(shape, shape, shape, jax.ShapeDtypeStruct((fsdp * rows, columns), jnp.bfloat16)),
            in_specs=[pl.BlockSpec(memory_space=pltpu.HBM)] * 4 + [pl.BlockSpec(memory_space=pl.ANY)] * 2,
            out_specs=[pl.BlockSpec(memory_space=pltpu.VMEM)] * 4,
            scratch_shapes=[
                block, block, block, block,
                pltpu.VMEM((8, LANES), jnp.float32),
                pltpu.VMEM((2 * tp - 1, 8, LANES), jnp.float32),
                pltpu.VMEM((8, LANES), jnp.float32),
                pltpu.VMEM((line - 1, 8, LANES), jnp.float32),
                pltpu.SMEM(step_count.shape, jnp.int32), pltpu.SMEM(tile_round.shape, jnp.int32),
                sems((6,)), sems((2 * tp - 1,)), sems((2 * tp - 1,)), sems((line - 1,)), sems((line - 1,)),
                sems((fsdp, count)), sems((fsdp, count)), sems((fsdp, count)), sems((fsdp, count)),
            ],
            compiler_params=pltpu.CompilerParams(
                collective_id=0, has_side_effects=True, vmem_limit_bytes=40 * 1024 * 1024),
        )(*[pltpu.with_memory_space_constraint(x, pltpu.HBM) for x in (
            gradients, master, first_moment, second_moment)], step_count, tile_round)
        results = (p, m, v, w)
        return pl.pallas_call(
            put_out,
            out_shape=tuple(jax.ShapeDtypeStruct(x.shape, x.dtype) for x in results),
            in_specs=[pl.BlockSpec(memory_space=pltpu.VMEM)] * 4,
            out_specs=[pl.BlockSpec(memory_space=pltpu.HBM)] * 4,
            scratch_shapes=[sems((4,))],
            compiler_params=pltpu.CompilerParams(vmem_limit_bytes=1024 * 1024),
        )(*results)

    return jax.shard_map(
        local,
        mesh=mesh,
        in_specs=(P("fsdp", "tp"), P("fsdp", "tp"), P("fsdp", "tp"), P("fsdp", "tp"), P(), P()),
        out_specs=(P("fsdp", "tp"), P("fsdp", "tp"), P("fsdp", "tp"), P(None, "tp")),
        check_vma=False,
    )
```

```python
import functools

import jax
import jax.numpy as jnp
from jax import lax
from jax.experimental import pallas as pl
from jax.experimental.pallas import tpu as pltpu
from jax.sharding import PartitionSpec as P

ROUNDS = 4
LANES = 128
MESH = pl.DeviceIdType.MESH

beta_one = 0.9
beta_two = 0.95
adam_epsilon = 1e-08
learning_rate = 0.01
weight_decay = 0.1
clip_norm = 1.0
square_limit = 1000000.0


def plan(fsdp, columns):
    if fsdp > 16 or columns % (16 * LANES):
        return [(0, columns, False)]
    unit = columns // 16
    chunks, start = [], 0
    for index, units in enumerate((4, 4, 4, 4)):
        chunks.append((start, units * unit, False))
        start += units * unit
    return chunks


def kernel(fsdp, tp, chunks, g_hbm, p_hbm, m_hbm, v_hbm, step_hbm, round_hbm,
           p_out, m_out, v_out, w_out,
           g_ref, p_ref, m_ref, v_ref, own_a, slots_a, own_b, slots_b,
           step_ref, round_ref, load_sem, sa_sem, ra_sem, sb_sem, rb_sem, up_sem, down_sem, side_sem, recv_sem):
    line = fsdp // 2
    f = lax.axis_index("fsdp")
    t = lax.axis_index("tp")
    a = f // 2
    b = f % 2
    rows, columns = g_ref.shape
    tile = rows // ROUNDS

    group = [(db, dt) for db in range(2) for dt in range(tp) if (db, dt) != (0, 0)]

    def peer_a(db, dt):
        return (a * 2 + (b + db) % 2, (t + dt) % tp)

    def peer_b(d):
        return (((a + d) % line) * 2 + b, t)

    loads = [pltpu.make_async_copy(src, dst, load_sem.at[i]) for i, (src, dst) in enumerate(
        ((g_hbm, g_ref), (round_hbm, round_ref), (step_hbm, step_ref),
         (p_hbm, p_ref), (m_hbm, m_ref), (v_hbm, v_ref)))]
    loads[0].start()
    barrier = pltpu.get_barrier_semaphore()
    for d in range(1, line):
        pl.semaphore_signal(barrier, inc=1, device_id=peer_b(d), device_id_type=MESH)
    for db, dt in group:
        pl.semaphore_signal(barrier, inc=1, device_id=peer_a(db, dt), device_id_type=MESH)
    for load in loads[1:]:
        load.start()

    row_ids = lax.broadcasted_iota(jnp.int32, (8, LANES), 0)
    loads[1].wait()
    mine = [round_ref[f * ROUNDS + k] for k in range(ROUNDS)]
    loads[0].wait()
    payload = jnp.zeros((8, LANES), jnp.float32)
    for k in range(ROUNDS):
        part = jnp.zeros((tile, LANES), jnp.float32)
        for c in range(columns // LANES):
            piece = g_ref[k * tile:(k + 1) * tile, c * LANES:(c + 1) * LANES]
            part = part + piece * piece
        part = jnp.sum(part, axis=0, keepdims=True)
        payload = payload + jnp.where(row_ids == mine[k], part, 0.0)
    own_a[...] = payload
    pl.semaphore_wait(barrier, len(group) + line - 1)

    sends_a = []
    for i, (db, dt) in enumerate(group):
        sends_a.append(pltpu.make_async_remote_copy(
            src_ref=own_a, dst_ref=slots_a.at[i], send_sem=sa_sem.at[i], recv_sem=ra_sem.at[i],
            device_id=peer_a(db, dt), device_id_type=MESH))
        sends_a[-1].start()
    for load in loads[2:]:
        load.wait()
    steps = jnp.full((1, LANES), step_ref[0].astype(jnp.float32), jnp.float32)
    inverse_one = 1.0 / (1.0 - jnp.exp(steps * jnp.log(jnp.float32(beta_one))))
    inverse_two = 1.0 / (1.0 - jnp.exp(steps * jnp.log(jnp.float32(beta_two))))
    inverse_one = inverse_one[:, :1]
    inverse_two = inverse_two[:, :1]
    total = payload
    for i, copy in enumerate(sends_a):
        copy.wait_recv()
        total = total + slots_a[i]
    own_b[...] = total
    sends_b = []
    for d in range(1, line):
        sends_b.append(pltpu.make_async_remote_copy(
            src_ref=own_b, dst_ref=slots_b.at[d - 1], send_sem=sb_sem.at[d - 1], recv_sem=rb_sem.at[d - 1],
            device_id=peer_b(d), device_id_type=MESH))
        sends_b[-1].start()
    for d, copy in enumerate(sends_b):
        copy.wait_recv()
        total = total + slots_b[d]

    scales, keeps = [], []
    for k in range(ROUNDS):
        picked = jnp.sum(jnp.where(row_ids == mine[k], total, 0.0), axis=0, keepdims=True)
        picked = jnp.sum(picked, axis=1, keepdims=True)
        keeps.append(picked >= square_limit)
        scales.append(jnp.minimum(1.0, clip_norm / (jnp.sqrt(picked) + 1e-06)))

    def block_of(row, c):
        start, width, _ = chunks[c]
        return w_out.at[pl.ds(pl.multiple_of(row * rows, rows), rows), pl.ds(start, width)]

    def send(row, c, sems, target):
        return pltpu.make_async_remote_copy(
            src_ref=block_of(row, c), dst_ref=block_of(row, c), send_sem=sems.at[row, c],
            recv_sem=recv_sem.at[row, c], device_id=(target, t), device_id_type=MESH)

    side = a * 2 + (1 - b)
    above, below = a < line - 1, a > 0

    def up(row, c):
        return send(row, c, up_sem, f + 2)

    def down(row, c):
        return send(row, c, down_sem, f - 2)

    def across(row, c):
        return send(row, c, side_sem, side)

    def when_do(condition, make, method):
        @pl.when(condition)
        def _():
            getattr(make(), method)()

    sent = []

    def go(condition, make):
        when_do(condition, make, "start")
        sent.append((condition, make))

    always = a >= 0
    for c, (start, width, first) in enumerate(chunks):
        for k in range(ROUNDS):
            at = (slice(k * tile, (k + 1) * tile), slice(start, start + width))
            old_p, old_m, old_v = p_ref[at], m_ref[at], v_ref[at]
            clipped = g_ref[at] * scales[k]
            moment = beta_one * old_m + (1.0 - beta_one) * clipped
            second = beta_two * old_v + (1.0 - beta_two) * clipped * clipped
            ratio = moment * inverse_one / (jnp.sqrt(second * inverse_two) + adam_epsilon)
            param = old_p - learning_rate * (ratio + weight_decay * old_p)
            param = jnp.where(keeps[k], old_p, param)
            p_out[at] = param
            m_out[at] = jnp.where(keeps[k], old_m, moment)
            v_out[at] = jnp.where(keeps[k], old_v, second)
        own_rows = pl.ds(pl.multiple_of(f * rows, rows), rows)
        w_out[own_rows, start:start + width] = p_out[:, start:start + width].astype(jnp.bfloat16)
        go(always, functools.partial(across, f, c))
        go(above, functools.partial(up, f, c))
        go(below, functools.partial(down, f, c))

    for c, (_, _, first) in enumerate(chunks):
        if first:
            across(side, c).wait_recv()
            go(above, functools.partial(up, side, c))
            go(below, functools.partial(down, side, c))

    for d in range(1, line):
        passing = [(False, c) for c in range(len(chunks))]
        passing += [(True, c) for c, (_, _, first) in enumerate(chunks) if first]
        for adopted, c in passing:
            for from_below in (True, False):
                inside = (a >= d) if from_below else (a + d <= line - 1)
                onward = above if from_below else below
                row = (side if adopted else f) + (-2 * d if from_below else 2 * d)
                make = functools.partial(up if from_below else down, row, c)
                when_do(inside, make, "wait_recv")
                go(jnp.logical_and(inside, onward), make)
                if not (adopted or chunks[c][2]):
                    go(inside, functools.partial(across, row, c))

    for c, (_, _, first) in enumerate(chunks):
        if not first:
            across(side, c).wait_recv()
    for d in range(1, line):
        for c, (_, _, first) in enumerate(chunks):
            if not first:
                when_do(a >= d, functools.partial(across, side - 2 * d, c), "wait_recv")
                when_do(a + d <= line - 1, functools.partial(across, side + 2 * d, c), "wait_recv")

    for copy in sends_a + sends_b:
        copy.wait_send()
    for condition, make in sent:
        when_do(condition, make, "wait_send")


def put_out(*refs):
    sources, targets, sem = refs[:4], refs[4:8], refs[8]
    copies = [pltpu.make_async_copy(src, dst, sem.at[i]) for i, (src, dst) in enumerate(zip(sources, targets))]
    for copy in reversed(copies):
        copy.start()
    for copy in copies:
        copy.wait()


def solution(mesh):
    fsdp, tp = mesh.shape["fsdp"], mesh.shape["tp"]

    def local(master, first_moment, second_moment, gradients, step_count, tile_round):
        rows, columns = master.shape
        chunks = plan(fsdp, columns)
        count = len(chunks)
        line = fsdp // 2
        shape = jax.ShapeDtypeStruct((rows, columns), jnp.float32)
        sems = pltpu.SemaphoreType.DMA
        block = pltpu.VMEM((rows, columns), jnp.float32)
        p, m, v, w = pl.pallas_call(
            functools.partial(kernel, fsdp, tp, chunks),
            out_shape=(shape, shape, shape, jax.ShapeDtypeStruct((fsdp * rows, columns), jnp.bfloat16)),
            in_specs=[pl.BlockSpec(memory_space=pltpu.HBM)] * 4 + [pl.BlockSpec(memory_space=pl.ANY), pl.BlockSpec(memory_space=pltpu.HBM)],
            out_specs=[pl.BlockSpec(memory_space=pltpu.VMEM)] * 4,
            scratch_shapes=[
                block, block, block, block,
                pltpu.VMEM((8, LANES), jnp.float32),
                pltpu.VMEM((2 * tp - 1, 8, LANES), jnp.float32),
                pltpu.VMEM((8, LANES), jnp.float32),
                pltpu.VMEM((line - 1, 8, LANES), jnp.float32),
                pltpu.SMEM(step_count.shape, jnp.int32), pltpu.SMEM(tile_round.shape, jnp.int32),
                sems((6,)), sems((2 * tp - 1,)), sems((2 * tp - 1,)), sems((line - 1,)), sems((line - 1,)),
                sems((fsdp, count)), sems((fsdp, count)), sems((fsdp, count)), sems((fsdp, count)),
            ],
            compiler_params=pltpu.CompilerParams(
                collective_id=0, has_side_effects=True, vmem_limit_bytes=40 * 1024 * 1024),
        )(*[pltpu.with_memory_space_constraint(x, pltpu.HBM) for x in (
            gradients, master, first_moment, second_moment)], step_count,
          pltpu.with_memory_space_constraint(tile_round, pltpu.HBM))
        results = (p, m, v, w)
        return pl.pallas_call(
            put_out,
            out_shape=tuple(jax.ShapeDtypeStruct(x.shape, x.dtype) for x in results),
            in_specs=[pl.BlockSpec(memory_space=pltpu.VMEM)] * 4,
            out_specs=[pl.BlockSpec(memory_space=pltpu.HBM)] * 4,
            scratch_shapes=[sems((4,))],
            compiler_params=pltpu.CompilerParams(vmem_limit_bytes=1024 * 1024),
        )(*results)

    return jax.shard_map(
        local,
        mesh=mesh,
        in_specs=(P("fsdp", "tp"), P("fsdp", "tp"), P("fsdp", "tp"), P("fsdp", "tp"), P(), P()),
        out_specs=(P("fsdp", "tp"), P("fsdp", "tp"), P("fsdp", "tp"), P(None, "tp")),
        check_vma=False,
    )
```
